32 devices in a mesh: groups: 2 (over y), ulysses: 4 (over z), blk: 2 (over x), handoff: 2 (over core).
Axes of the slice: x: 2, y: 2, z: 4, core: 2. Of those that a mesh axis runs over, the one named last changes fastest.
Arguments:
- queries: bfloat16 [4, 512, 4096], P(('groups', 'handoff'), ('blk', 'ulysses')), parts along dimension 0, may hold values from -24 to 24
- keys: bfloat16 [4, 512, 2048], P(('groups', 'handoff'), ('blk', 'ulysses')), parts along dimension 0, may hold values from -7.5 to 7.5
- values: bfloat16 [4, 512, 2048], P(('groups', 'handoff'), ('blk', 'ulysses')), parts along dimension 0, may hold values from -6 to 6
- request_pages: int32 [4, 4], P('groups'), parts along dimension 0, may hold values from 1 to 4, 8 in all within a row
- page_table: int32 [4, 8], P('groups'), parts along dimension 0, may hold values from 0 to 15, as said below
Outputs:
- attended: bfloat16 [4, 512, 4096], P(('groups', 'handoff'), ('blk', 'ulysses')), parts along dimension 0
- cache_keys: bfloat16 [32, 16, 64, 128], P(('groups', 'blk', 'handoff'), 'ulysses'), parts along dimension 0
- cache_values: bfloat16 [32, 16, 64, 128], P(('groups', 'blk', 'handoff'), 'ulysses'), parts along dimension 0
The draws below stay inside these ranges and needn't reach their ends.
There are 2 independent parts, one for each index of `groups`. The reference program is written for one: setup_inputs(seed, part) draws one part's arguments, and reference() takes and returns one part's arrays. A program takes and returns all parts, laid end to end along the dimension named above; each array names one. Nothing has to cross between parts.
Inputs may be any that keep to these rules, and one draw needn't show every extreme that they name: `request_pages`: A pack's 4 requests fill its 8 pages; the longest holds exactly 4 of them. `page_table`: all rows together name every pool page once; the 4 pages of each aligned run of 4 pages of a pack's row go in equal numbers to each aligned run of 4 pool pages.
All inputs are finite; a program needn't handle non-finite values.
Results may differ from the reference program's by a relative error of at most 0.012.
Values may be sent and summed in bfloat16 or wider, within the bound.
No kernel may reach another device: no remote copies, remote signals or barrier semaphores. Data moves between devices by JAX's collectives and lax.ppermute only.
A program may use at most 64 MiB of HBM per device.

```python
import math
import jax
import jax.numpy as jnp
import numpy as np
from jax import lax

QH = 32
KVH = 16
HD = 128
WINDOW = 4096
PAGE = 64
REQS = 4
SEQ = 512
PACKS = 2
PACK_PAGES = 8
SHARD_PAGES = 4
POOL = 16


def draw_queries(key, part):
    normal = jax.random.normal(jax.random.fold_in(key, 11), (PACKS, SEQ, QH * HD), jnp.float32)
    scaled = normal * 4.0
    return jnp.clip(scaled, -24.0, 24.0).astype(jnp.bfloat16)


def draw_page_table(key, part):
    slots_dev = SHARD_PAGES
    sources = POOL // SHARD_PAGES
    per_peer = slots_dev // sources
    lane_ids = jnp.arange(slots_dev, dtype=jnp.int32)[None, :]
    noise_one = jax.random.randint(jax.random.fold_in(key, 21), (sources, slots_dev), 0, 1 << 20) * slots_dev + lane_ids
    noise_two = jax.random.randint(jax.random.fold_in(key, 22), (sources, slots_dev), 0, 1 << 20) * slots_dev + lane_ids
    first_perm = jnp.argsort(noise_one, axis=1).astype(jnp.int32)
    second_perm = jnp.argsort(noise_two, axis=1).astype(jnp.int32)
    target = first_perm // per_peer
    within = first_perm % per_peer
    source_ids = jnp.arange(sources, dtype=jnp.int32)[:, None]
    slot_index = second_perm[target, source_ids * per_peer + within]
    pool_page = target * slots_dev + slot_index
    blk_lanes = sources // PACKS
    return jnp.transpose(pool_page.reshape(blk_lanes, PACKS, slots_dev), (1, 0, 2)).reshape(PACKS, PACK_PAGES).astype(jnp.int32)


def levels(stream_key, extent, shards, smallest, largest):
    def one(position, shards_of):
        heights = jax.random.uniform(jax.random.fold_in(jax.random.fold_in(stream_key, 6), position), (shards_of,), jnp.float32, smallest / len(shards), largest / len(shards))
        return jnp.repeat(jnp.exp(heights), extent[position] // shards_of).reshape((-1,) + (1,) * (len(extent) - position - 1))

    gain = one(*shards[0])
    for cut in shards[1:]:
        gain = gain * one(*cut)
    return gain


def split_up(count, total, most, skew):
    portions = [(1 << 20) // math.isqrt(standing ** skew) + 1 for standing in range(2, count + 1)]
    surplus, holding = total - most - (count - 1), [1] * (count - 1)
    while surplus > 0:
        movable = [i for i in range(count - 1) if holding[i] < most]
        pool, budget = sum([portions[i] for i in movable]), surplus
        for i in movable:
            extra = min(most - holding[i], max(1, budget * portions[i] // pool), surplus)
            holding[i] = holding[i] + extra
            surplus = surplus - extra
    return np.array([most] + holding)


def ragged(own_key, amount, total, limit, slope):
    if amount == 2:
        one = jax.random.randint(own_key, (), max(1, total - limit), min(limit, total - 1) + 1)
        return jnp.stack([one, total - one])
    lengths = jnp.asarray(split_up(amount, total, limit, slope), jnp.int32)
    twos = (amount - 1) // 2
    giver, receiver = lengths[1:1 + 2 * twos:2], lengths[2:2 + 2 * twos:2]
    slack = jnp.minimum(giver - 1, limit - receiver)
    moved = jax.random.randint(jax.random.fold_in(own_key, 1), (twos,), 0, 1 << 20) % (slack + 1)
    lengths = lengths.at[1:1 + 2 * twos:2].set(giver - moved).at[2:2 + 2 * twos:2].set(receiver + moved)
    return lengths[jax.random.permutation(jax.random.fold_in(own_key, 2), amount)]


def scatter_about(stream_key, dims, width, limit, pieces=(), kind=jnp.bfloat16):
    level = levels(stream_key, dims, pieces, -0.22, 0.18) if pieces else 1.0
    array = jax.random.normal(stream_key, dims, jnp.float32) * width * level
    return jnp.minimum(jnp.maximum(array, -limit), limit).astype(kind)


def setup_inputs(seed: int = 0, part: int = 0) -> dict:
    key_list = jax.random.split(jax.random.key(seed), 6)
    part_splits = jax.random.split(jax.random.fold_in(key_list[5], part), 6)
    queries = draw_queries(jax.random.fold_in(jax.random.fold_in(key_list[5], part), 71), part)
    keys = scatter_about(part_splits[1], (PACKS, SEQ, KVH * HD), 1.25, 7.5, ((0, 2), (1, 8)))
    values = scatter_about(part_splits[2], (PACKS, SEQ, KVH * HD), 1.0, 6.0, ((0, 2), (1, 8)))
    request_pages = jax.vmap(lambda own: ragged(own, REQS, PACK_PAGES, PACK_PAGES // 2, 1))(jax.random.split(part_splits[3], PACKS)).reshape((PACKS, REQS)).astype(jnp.int32)
    page_table = draw_page_table(jax.random.fold_in(jax.random.fold_in(key_list[5], part), 71), part)
    return dict(queries=queries, keys=keys, values=values, request_pages=request_pages, page_table=page_table)


QUERY_SCALE = 144.0 ** -0.5
SOFT_CAP = 50.0
ROPE_BASE = 10000.0


def request_marks(pages_row, positions):
    request_ends = jnp.cumsum(pages_row, dtype=jnp.int32) * PAGE
    request_starts = request_ends - pages_row * PAGE
    owner_index = jnp.sum((positions[:, None] >= request_ends[None, :]).astype(jnp.int32), axis=1)
    first_token = jnp.max(jnp.where(positions[:, None] >= request_starts[None, :], request_starts[None, :], 0), axis=1)
    return owner_index.astype(jnp.int32), (positions - first_token).astype(jnp.int32)


def rotate(head_rows, offsets):
    head_width = head_rows.shape[-1]
    half_width = head_width // 2
    frequency = ROPE_BASE ** (-(2.0 * jnp.arange(half_width, dtype=jnp.float32)) / head_width)
    angles = offsets.astype(jnp.float32)[:, None] * frequency[None, :]
    cosine = jnp.cos(angles)[:, None, :]
    sines = jnp.sin(angles)[:, None, :]
    as_float = head_rows.astype(jnp.float32)
    front_half = as_float[..., :half_width]
    back_half = as_float[..., half_width:]
    turned = jnp.concatenate([front_half * cosine - back_half * sines, back_half * cosine + front_half * sines], axis=-1)
    return turned.astype(jnp.bfloat16)


def reference(queries, keys, values, request_pages, page_table):
    group_size = QH // KVH
    block_rows = math.gcd(SEQ, 512)
    key_span = WINDOW + block_rows
    positions = jnp.arange(SEQ, dtype=jnp.int32)
    pad_positions = jnp.arange(SEQ + WINDOW, dtype=jnp.int32) - WINDOW
    outputs = []
    key_pages = []
    value_pages = []
    for pack_index in range(PACKS):
        owner_all, offsets = request_marks(request_pages[pack_index], positions)
        pad_owner, unused_offsets = request_marks(request_pages[pack_index], pad_positions)
        query_turned = rotate(queries[pack_index].reshape(SEQ, QH, HD), offsets)
        key_turned = rotate(keys[pack_index].reshape(SEQ, KVH, HD), offsets)
        value_heads = values[pack_index].reshape(SEQ, KVH, HD)
        pad_keys = jnp.concatenate([jnp.zeros((WINDOW, KVH, HD), jnp.bfloat16), key_turned], axis=0)
        pad_values = jnp.concatenate([jnp.zeros((WINDOW, KVH, HD), jnp.bfloat16), value_heads], axis=0)

        def attend(offset):
            query_block = lax.dynamic_slice_in_dim(query_turned, offset, block_rows, 0).astype(jnp.float32)
            query_block = query_block.reshape(block_rows, KVH, group_size, HD)
            key_block = lax.dynamic_slice_in_dim(pad_keys, offset, key_span, 0).astype(jnp.float32)
            value_block = lax.dynamic_slice_in_dim(pad_values, offset, key_span, 0).astype(jnp.float32)
            scores = jnp.einsum("qgrd,kgd->gqrk", query_block, key_block, precision=lax.Precision.HIGHEST) * QUERY_SCALE
            capped = SOFT_CAP * jnp.tanh(scores / SOFT_CAP)
            query_pos = lax.dynamic_slice_in_dim(positions, offset, block_rows)
            query_owner = lax.dynamic_slice_in_dim(owner_all, offset, block_rows)
            key_pos = lax.dynamic_slice_in_dim(pad_positions, offset, key_span)
            key_owner = lax.dynamic_slice_in_dim(pad_owner, offset, key_span)
            distance = query_pos[:, None] - key_pos[None, :]
            allowed = (query_owner[:, None] == key_owner[None, :]) & (distance >= 0) & (distance < WINDOW) & (key_pos[None, :] >= 0)
            weights = jnp.where(allowed[None, :, None, :], jnp.exp(capped), jnp.float32(0.0))
            totals = jnp.sum(weights, axis=-1)
            rounded = lax.optimization_barrier(weights.astype(jnp.bfloat16)).astype(jnp.float32)
            mixture = jnp.einsum("gqrk,kgd->qgrd", rounded, value_block, precision=lax.Precision.HIGHEST)
            return (mixture / jnp.transpose(totals, (1, 0, 2))[..., None]).astype(jnp.bfloat16)

        starts = jnp.arange(SEQ // block_rows, dtype=jnp.int32) * block_rows
        blocks = lax.map(attend, starts)
        outputs.append(blocks.reshape(SEQ, QH * HD))
        key_pages.append(key_turned.reshape(PACK_PAGES, PAGE, KVH, HD))
        value_pages.append(value_heads.reshape(PACK_PAGES, PAGE, KVH, HD))
    attended = jnp.stack(outputs)
    flat_keys = jnp.transpose(jnp.concatenate(key_pages, axis=0), (0, 2, 1, 3))
    flat_values = jnp.transpose(jnp.concatenate(value_pages, axis=0), (0, 2, 1, 3))
    pool_slots = page_table.reshape(-1).astype(jnp.int32)
    cache_keys = jnp.zeros_like(flat_keys).at[pool_slots].set(flat_keys)
    cache_values = jnp.zeros_like(flat_values).at[pool_slots].set(flat_values)
    return attended, cache_keys, cache_values
```

```python
import functools
import math

import jax
import jax.numpy as jnp
from jax import lax
from jax.experimental import pallas as pl
from jax.experimental.pallas import tpu as pltpu
from jax.sharding import PartitionSpec as P

QH = 32
KVH = 16
HD = 128
WINDOW = 4096
PAGE = 64

QUERY_SCALE = 144.0 ** (-0.5)
SOFT_CAP = 50.0
ROPE_BASE = 10000.0


VMEM = pltpu.VMEM
SMEM = pltpu.SMEM


def document_start(pages_ref, pack, page):
    start = jnp.int32(0)
    end = jnp.int32(0)
    for r in range(pages_ref.shape[1]):
        end = end + pages_ref[pack, r]
        start = jnp.where(page >= end, end, start)
    return start


def rope_tables(first_row, rows):
    lane = lax.broadcasted_iota(jnp.int32, (rows, HD), 1)
    row = lax.broadcasted_iota(jnp.int32, (rows, HD), 0) + first_row
    half = HD // 2
    exponent = (-2.0 * (lane % half).astype(jnp.float32)) / HD
    frequency = jnp.exp(exponent * math.log(ROPE_BASE))
    angles = row.astype(jnp.float32) * frequency
    sines = jnp.sin(angles)
    return jnp.cos(angles), jnp.where(lane < half, -sines, sines)


def rotate(head, cosine, sine):
    x = head.astype(jnp.float32)
    return (x * cosine + pltpu.roll(x, HD // 2, 1) * sine).astype(jnp.bfloat16)


def pack_kernel(ids_ref, pages_ref, *refs, ulysses, tensors):
    ins, outs = refs[: len(tensors)], refs[len(tensors):]
    u, x, pack = ids_ref[0], ids_ref[1], ids_ref[2]
    page = x * ulysses + u
    rows = ins[0].shape[1]
    first_row = (page - document_start(pages_ref, pack, page)) * PAGE
    cosine, sine = rope_tables(first_row, rows)
    for d in range(ulysses):
        peer = u ^ d
        column = 0
        for ref, turned in zip(ins, tensors):
            width = ref.shape[2] // ulysses
            for h in range(width // HD):
                source = pl.multiple_of(peer * width + h * HD, HD)
                head = ref[0, :, pl.ds(source, HD)]
                if turned:
                    head = rotate(head, cosine, sine)
                outs[d][:, column:column + HD] = head
                column += HD


def matching_page(table_ref, pack, first, count, target, target_pages, rank):
    found = jnp.int32(0)
    seen = jnp.int32(0)
    for j in range(count):
        match = lax.div(table_ref[pack, first + j], jnp.int32(target_pages)) == target
        found = jnp.where(match & (seen == rank), first + j, found)
        seen = seen + match.astype(jnp.int32)
    return found


def table_kernel(ids_ref, table_ref, *refs, ulysses, blocks, cores, groups):
    ins = refs[: len(groups)]
    kv_ref = refs[len(groups)]
    sends = refs[len(groups) + 1:]
    u, x, core = ids_ref[0], ids_ref[1], ids_ref[2]
    for ref, (e, first, count) in zip(ins, groups):
        for n in range(count):
            row = pl.multiple_of(((x ^ e) * ulysses + (u ^ (first + n))) * PAGE, PAGE)
            kv_ref[pl.ds(row, PAGE), :] = ref[n]
    per_peer = ulysses // (blocks * cores)
    for f in range(1, cores):
        target = x * cores + (core ^ f)
        for b in range(blocks):
            for r in range(per_peer):
                g = matching_page(table_ref, core, b * ulysses, ulysses, target, ulysses, r)
                row = pl.multiple_of(g * PAGE, PAGE)
                sends[f - 1][b * per_peer + r] = kv_ref[pl.ds(row, PAGE), :]


def cache_kernel(ids_ref, table_ref, kv_ref, *refs, ulysses, blocks, cores):
    received = refs[: cores - 1]
    keys_ref, values_ref = refs[cores - 1:]
    x, core = ids_ref[1], ids_ref[2]
    target = x * cores + core
    heads = keys_ref.shape[1]
    per_peer = ulysses // (blocks * cores)
    for f in range(cores):
        pack = core ^ f
        for b in range(blocks):
            for r in range(per_peer):
                g = matching_page(table_ref, pack, b * ulysses, ulysses, target, ulysses, r)
                slot = table_ref[pack, g] - target * ulysses
                if f == 0:
                    row = pl.multiple_of(g * PAGE, PAGE)
                    page = kv_ref[pl.ds(row, PAGE), :]
                else:
                    page = received[f - 1][b * per_peer + r]
                for h in range(heads):
                    keys_ref[slot, h] = page[:, h * HD:(h + 1) * HD]
                    values_ref[slot, h] = page[:, (heads + h) * HD:(heads + h + 1) * HD]


def attend_kernel(ids_ref, pages_ref, q_ref, kv_ref, out_ref, *, distance, ulysses, span, step):
    u, x, pack = ids_ref[0], ids_ref[1], ids_ref[2]
    page = x * ulysses + (u ^ distance)
    start = document_start(pages_ref, pack, page)
    span_pages = span // PAGE
    window_page = jnp.maximum(page - (span_pages - 1), 0)
    kv_local = kv_ref.shape[1] // (2 * HD)
    group = q_ref.shape[1] // (kv_local * HD)
    rows = group * PAGE
    q_pos = page * PAGE + lax.broadcasted_iota(jnp.int32, (rows, step), 0) % PAGE
    lane = lax.broadcasted_iota(jnp.int32, (rows, step), 1)
    sequence = kv_ref.shape[0]
    for h in range(kv_local):
        first = h * group * HD
        q = jnp.concatenate(
            [q_ref[:, first + r * HD:first + (r + 1) * HD] for r in range(group)], axis=0
        )

        def block(n, carry, h=h, q=q):
            total, mixture = carry
            row = pl.multiple_of(window_page * PAGE + n * step, PAGE)
            keys = kv_ref[pl.ds(row, step), h * HD:(h + 1) * HD]
            values = kv_ref[pl.ds(row, step), (kv_local + h) * HD:(kv_local + h + 1) * HD]
            scores = lax.dot_general(
                q, keys, (((1,), (1,)), ((), ())), preferred_element_type=jnp.float32
            )
            capped = jnp.tanh(scores * (QUERY_SCALE / SOFT_CAP)) * (SOFT_CAP * math.log2(math.e))
            k_pos = lane + row
            allowed = (k_pos <= q_pos) & (k_pos >= start * PAGE)
            if sequence > WINDOW:
                allowed = allowed & (q_pos - k_pos < WINDOW)
            weights = jnp.where(allowed, jnp.exp2(capped), 0.0)
            total = total + jnp.sum(weights, axis=1, keepdims=True)
            mixture = mixture + jnp.dot(
                weights.astype(jnp.bfloat16), values, preferred_element_type=jnp.float32
            )
            return total, mixture

        carry = (jnp.zeros((rows, 1), jnp.float32), jnp.zeros((rows, HD), jnp.float32))
        if span == step:
            total, mixture = block(0, carry)
        else:
            total, mixture = lax.fori_loop(0, span // step, block, carry)
        result = (mixture / total).astype(jnp.bfloat16)
        for r in range(group):
            out_ref[:, first + r * HD:first + (r + 1) * HD] = result[r * PAGE:(r + 1) * PAGE]


def gather_kernel(ids_ref, *refs, ulysses):
    ins, out_ref = refs[:ulysses], refs[ulysses]
    u = ids_ref[0]
    width = ins[0].shape[1]
    for d in range(ulysses):
        column = pl.multiple_of((u ^ d) * width, HD)
        out_ref[0, :, pl.ds(column, width)] = ins[d][...]


def call(kernel, scalars, arrays, outs, name):
    return pl.pallas_call(
        kernel,
        in_specs=[pl.BlockSpec(memory_space=SMEM)] * len(scalars)
        + [pl.BlockSpec(memory_space=VMEM)] * len(arrays),
        out_specs=[pl.BlockSpec(memory_space=VMEM)] * len(outs),
        out_shape=[jax.ShapeDtypeStruct(s, jnp.bfloat16) for s in outs],
        name=name,
    )(*scalars, *arrays)


def swap(array, axis, distance):
    route = [(i, i ^ distance) for i in range(lax.axis_size(axis))]
    return lax.ppermute(array, axis, route)


def body(queries, keys, values, request_pages, page_table):
    rows = queries.shape[1]
    ulysses = lax.axis_size("ulysses")
    blocks = lax.axis_size("blk")
    cores = lax.axis_size("handoff")
    kv_local = KVH // ulysses
    q_width = (QH // ulysses) * HD
    kv_width = 2 * kv_local * HD
    pages = ulysses * blocks
    span = pages // 2 * PAGE
    step = math.gcd(span, 256)
    ids = jnp.stack(
        [lax.axis_index("ulysses"), lax.axis_index("blk"), lax.axis_index("handoff")]
    ).astype(jnp.int32)

    kv_out = call(
        functools.partial(pack_kernel, ulysses=ulysses, tensors=(True, False)),
        (ids, request_pages), (keys, values), [(rows, kv_width)] * ulysses, "pack_kv",
    )
    kv_here = [kv_out[0]] + [swap(kv_out[d], "ulysses", d) for d in range(1, ulysses)]
    q_out = call(
        functools.partial(pack_kernel, ulysses=ulysses, tensors=(True,)),
        (ids, request_pages), (queries,), [(rows, q_width)] * ulysses, "pack_q",
    )
    q_here = [q_out[0]] + [swap(q_out[d], "ulysses", d) for d in range(1, ulysses)]

    if ulysses * (blocks - 1) <= 8:
        parts = [(d, kv[None]) for d, kv in enumerate(kv_here)]
    else:
        parts = [(0, jnp.stack(kv_here))]
    groups, tables = [], []
    for e in range(blocks):
        for first, part in parts:
            groups.append((e, first, part.shape[0]))
            tables.append(part if e == 0 else swap(part, "blk", e))
    per_core = blocks * (ulysses // (blocks * cores))
    kv_table, *sends = call(
        functools.partial(
            table_kernel, ulysses=ulysses, blocks=blocks, cores=cores, groups=tuple(groups)
        ),
        (ids, page_table), tables,
        [(pages * PAGE, kv_width)] + [(per_core, PAGE, kv_width)] * (cores - 1), "table",
    )
    received = [swap(s, "handoff", f + 1) for f, s in enumerate(sends)]

    merged = [None] * ulysses
    for d in list(range(1, ulysses)) + [0]:
        (page_out,) = call(
            functools.partial(
                attend_kernel, distance=d, ulysses=ulysses, span=span, step=step
            ),
            (ids, request_pages), (q_here[d], kv_table), [(rows, q_width)], "attend",
        )
        merged[d] = swap(page_out, "ulysses", d) if d else page_out
    cache_keys, cache_values = call(
        functools.partial(cache_kernel, ulysses=ulysses, blocks=blocks, cores=cores),
        (ids, page_table), [kv_table] + received, [(ulysses, kv_local, PAGE, HD)] * 2, "cache",
    )
    (attended,) = call(
        functools.partial(gather_kernel, ulysses=ulysses),
        (ids,), merged, [(1, rows, QH * HD)], "gather",
    )
    return attended, cache_keys, cache_values


def solution(mesh):
    tokens = P(("groups", "handoff"), ("blk", "ulysses"), None)
    pool = P(("groups", "blk", "handoff"), "ulysses", None, None)
    return jax.shard_map(
        body,
        mesh=mesh,
        in_specs=(tokens, tokens, tokens, P("groups", None), P("groups", None)),
        out_specs=(tokens, pool, pool),
        check_vma=False,
    )
```
